16 devices in a mesh: dp: 4 (over z, y), ep: 4 (over x, core).
Axes of the slice: x: 2, y: 2, z: 2, core: 2. Of those that a mesh axis runs over, the one named last changes fastest.
Arguments:
- tokens: bfloat16 [4096, 2048], P(('dp', 'ep')), parts along dimension 0
- expert_ids: int32 [4096, 4], P(('dp', 'ep')), parts along dimension 0
- gate_vals: float32 [4096, 4], P(('dp', 'ep')), parts along dimension 0
- w_gate: bfloat16 [60, 2048, 1408], P('ep')
- w_up: bfloat16 [60, 2048, 1408], P('ep')
- w_down: bfloat16 [60, 1408, 2048], P('ep')
- shared_gate: bfloat16 [2048, 5632], replicated
- shared_up: bfloat16 [2048, 5632], replicated
- shared_down: bfloat16 [5632, 2048], replicated
Outputs:
- output: bfloat16 [4096, 2048], P(('dp', 'ep')), parts along dimension 0
There are 4 independent parts. The reference program is written for one: setup_inputs(seed, part) draws one part's arguments, and reference() takes and returns one part's arrays. A program takes and returns all parts, laid end to end along the dimension named above; an argument that names none is the same for every part.
All inputs are finite; a program needn't handle non-finite values.
Results may differ from the reference program's by a relative error of at most 0.00670956.
Values are sent between devices in bfloat16 or wider.
A program may use at most 1.25 GiB of HBM per device.

```python
import jax
import jax.numpy as jnp
from jax import lax

GROUP_SIZE = 4
TOKENS_DEV = 256
MODEL_DIM = 2048
EXPERT_FF = 1408
SHARED_FF = 5632
EXPERTS = 60
TOP_K = 4
LOCAL_EXPERTS = EXPERTS // GROUP_SIZE
SPREAD_SLOTS = max(GROUP_SIZE, EXPERTS // 2)
CAPACITY = (TOKENS_DEV * TOP_K + SPREAD_SLOTS - 1) // SPREAD_SLOTS


def route_ids(route_key):
    key_shift, key_base, key_perm = jax.random.split(route_key, 3)
    dev_shift = jax.random.randint(key_shift, (GROUP_SIZE, 1, 1), 0, GROUP_SIZE)
    base_local = jax.random.randint(key_base, (), 0, LOCAL_EXPERTS)
    src_index = jnp.arange(GROUP_SIZE, dtype=jnp.int32).reshape(GROUP_SIZE, 1, 1)
    local_shift = base_local + src_index * (SPREAD_SLOTS // GROUP_SIZE)
    perm_keys = jax.random.split(key_perm, GROUP_SIZE)
    tok_order = jax.vmap(lambda perm_key: jax.random.permutation(perm_key, TOKENS_DEV))(perm_keys)
    row_pos = tok_order[:, :, None] * TOP_K + jnp.arange(TOP_K, dtype=jnp.int32).reshape(1, 1, TOP_K)
    spot_idx = row_pos % SPREAD_SLOTS
    dest_dev = (dev_shift + spot_idx) % GROUP_SIZE
    local_id = (local_shift + spot_idx // GROUP_SIZE) % LOCAL_EXPERTS
    return (dest_dev * LOCAL_EXPERTS + local_id).reshape(GROUP_SIZE * TOKENS_DEV, TOP_K).astype(jnp.int32)


def setup_inputs(seed: int = 0, part: int = 0) -> dict:
    part_key = jax.random.fold_in(jax.random.key(seed), part)
    key_tok, key_route, key_gate = jax.random.split(part_key, 3)
    weight_keys = jax.random.split(jax.random.key(seed + 1), 6)
    row_count = GROUP_SIZE * TOKENS_DEV
    tokens = jax.random.normal(key_tok, (row_count, MODEL_DIM), jnp.float32).astype(jnp.bfloat16)
    expert_ids = route_ids(key_route)
    gate_vals = 3.0 * TOP_K ** -0.5 * jax.nn.sigmoid(2.0 * jax.random.normal(key_gate, (row_count, TOP_K), jnp.float32))
    w_gate = (jax.random.normal(weight_keys[0], (EXPERTS, MODEL_DIM, EXPERT_FF), jnp.float32) * MODEL_DIM ** -0.5).astype(jnp.bfloat16)
    w_up = (jax.random.normal(weight_keys[1], (EXPERTS, MODEL_DIM, EXPERT_FF), jnp.float32) * MODEL_DIM ** -0.5).astype(jnp.bfloat16)
    w_down = (jax.random.normal(weight_keys[2], (EXPERTS, EXPERT_FF, MODEL_DIM), jnp.float32) * EXPERT_FF ** -0.5).astype(jnp.bfloat16)
    shared_gate = (jax.random.normal(weight_keys[3], (MODEL_DIM, SHARED_FF), jnp.float32) * MODEL_DIM ** -0.5).astype(jnp.bfloat16)
    shared_up = (jax.random.normal(weight_keys[4], (MODEL_DIM, SHARED_FF), jnp.float32) * MODEL_DIM ** -0.5).astype(jnp.bfloat16)
    shared_down = (jax.random.normal(weight_keys[5], (SHARED_FF, MODEL_DIM), jnp.float32) * SHARED_FF ** -0.5).astype(jnp.bfloat16)
    return {"tokens": tokens, "expert_ids": expert_ids, "gate_vals": gate_vals, "w_gate": w_gate, "w_up": w_up, "w_down": w_down, "shared_gate": shared_gate, "shared_up": shared_up, "shared_down": shared_down}


def swiglu(row_block, gate_w, up_w, down_w):
    gate_act = jnp.dot(row_block, gate_w, preferred_element_type=jnp.float32)
    up_act = jnp.dot(row_block, up_w, preferred_element_type=jnp.float32)
    hidden = (jax.nn.silu(gate_act) * up_act).astype(jnp.bfloat16)
    return jnp.dot(hidden, down_w, preferred_element_type=jnp.float32).astype(jnp.bfloat16)


def reference(tokens, expert_ids, gate_vals, w_gate, w_up, w_down, shared_gate, shared_up, shared_down):
    row_count = GROUP_SIZE * TOKENS_DEV
    src_ids = expert_ids.reshape(GROUP_SIZE, TOKENS_DEV * TOP_K)
    one_hot = (src_ids[:, :, None] == jnp.arange(EXPERTS, dtype=jnp.int32)[None, None, :]).astype(jnp.int32)
    slot_pos = jnp.sum(jnp.cumsum(one_hot, axis=1) * one_hot, axis=2) - 1
    buf_row = (jnp.arange(GROUP_SIZE, dtype=jnp.int32)[:, None] * CAPACITY + slot_pos).reshape(-1)
    flat_ids = src_ids.reshape(-1)
    token_rows = jnp.repeat(tokens, TOP_K, axis=0)
    buffers = jnp.zeros((EXPERTS, GROUP_SIZE * CAPACITY, MODEL_DIM), jnp.bfloat16)
    buffers = buffers.at[flat_ids, buf_row].set(token_rows)
    expert_out = lax.map(lambda operands: swiglu(operands[0], operands[1], operands[2], operands[3]), (buffers, w_gate, w_up, w_down))
    picked = expert_out[flat_ids, buf_row].reshape(row_count, TOP_K, MODEL_DIM)
    result_acc = tokens.astype(jnp.float32)
    for slot_idx in range(TOP_K):
        result_acc = result_acc + gate_vals[:, slot_idx:slot_idx + 1] * picked[:, slot_idx, :].astype(jnp.float32)
    shared_out = swiglu(tokens, shared_gate, shared_up, shared_down)
    return (result_acc + shared_out.astype(jnp.float32)).astype(jnp.bfloat16)
```

```python
import functools

import jax
import jax.numpy as jnp
from jax import lax
from jax.experimental import pallas as pl
from jax.experimental.pallas import tpu as pltpu
from jax.sharding import PartitionSpec as P

MESH = pl.DeviceIdType.MESH
F32 = jnp.float32
BF16 = jnp.bfloat16

GROUP = 4
CHUNK = 512
SLOTS = 40
EGROUP = 5
RING1 = 3
RING2 = 4
COVER = 2


def dot(a, b):
    return jnp.dot(a, b, preferred_element_type=F32)


def pieces(width):
    return [(start, min(256, width - start)) for start in range(0, width, 256)]


def moe_kernel(dims, ids_ref, gat_ref, tok, w_gate, w_up, w_down, s_gate, s_up, s_down, out,
               ring_g, ring_u, ring_d, acc, sacc, xall, xdf, xd, ybuf, hid, shid, gmat, pmat,
               recv_f, recv_p, recv_q, out_v, meta_loc, meta_all,
               sem_g, sem_u, sem_d, sem_x, sem_o, meta_s, meta_r,
               xq_s, xq_r, xp_s, xp_r, xf_s, xf_r, cf_s, cf_r, cp_s, cp_r, cq_s, cq_r):
    T, D, F, L, NS = dims
    KC = D // CHUNK
    ROWS = GROUP * SLOTS
    NGRP = L // EGROUP
    me = lax.axis_index("ep")
    pp = me + 1 - 2 * lax.rem(me, 2)
    qq = lax.rem(me + 2, GROUP)
    rr = lax.rem(pp + 2, GROUP)

    def remote(src, dst, s_sem, r_sem, dev):
        return pltpu.make_async_remote_copy(src_ref=src, dst_ref=dst, send_sem=s_sem, recv_sem=r_sem,
                                            device_id={"ep": dev}, device_id_type=MESH)

    n_cover = COVER * KC
    n_routed = L * KC
    n_gu = NS * KC + n_routed

    def gu_shared(idx, slot):
        i, k = idx // KC, lax.rem(idx, KC)
        rows, cols = pl.ds(pl.multiple_of(k * CHUNK, CHUNK), CHUNK), pl.ds(pl.multiple_of(i * F, 128), F)
        pltpu.make_async_copy(s_gate.at[rows, cols], ring_g.at[slot], sem_g.at[slot]).start()
        pltpu.make_async_copy(s_up.at[rows, cols], ring_u.at[slot], sem_u.at[slot]).start()

    def issue_gu(g, limit):
        slot = lax.rem(g, RING1)

        @pl.when(jnp.logical_and(g < n_cover, g < limit))
        def _():
            gu_shared(g, slot)

        @pl.when(jnp.logical_and(jnp.logical_and(g >= n_cover, g < n_cover + n_routed), g < limit))
        def _():
            r = g - n_cover
            per = KC * EGROUP
            grp, rest = r // per, lax.rem(r, per)
            k, e = rest // EGROUP, grp * EGROUP + lax.rem(rest, EGROUP)
            rows = pl.ds(pl.multiple_of(k * CHUNK, CHUNK), CHUNK)
            pltpu.make_async_copy(w_gate.at[e, rows, :], ring_g.at[slot], sem_g.at[slot]).start()
            pltpu.make_async_copy(w_up.at[e, rows, :], ring_u.at[slot], sem_u.at[slot]).start()

        @pl.when(jnp.logical_and(g >= n_cover + n_routed, g < limit))
        def _():
            gu_shared(g - n_routed, slot)

    def wait_gu(slot):
        pltpu.make_async_copy(w_gate.at[0, pl.ds(0, CHUNK), :], ring_g.at[slot], sem_g.at[slot]).wait()
        pltpu.make_async_copy(w_up.at[0, pl.ds(0, CHUNK), :], ring_u.at[slot], sem_u.at[slot]).wait()

    n_down = KC * L
    n_dn = n_down + KC * NS

    def issue_dn(t, limit):
        slot = lax.rem(t, RING2)

        @pl.when(jnp.logical_and(t < n_down, t < limit))
        def _():
            n, e = t // L, lax.rem(t, L)
            cols = pl.ds(pl.multiple_of(n * CHUNK, CHUNK), CHUNK)
            pltpu.make_async_copy(w_down.at[e, :, cols], ring_d.at[slot], sem_d.at[slot]).start()

        @pl.when(jnp.logical_and(t >= n_down, t < limit))
        def _():
            n, i = (t - n_down) // NS, lax.rem(t - n_down, NS)
            cols = pl.ds(pl.multiple_of(n * CHUNK, CHUNK), CHUNK)
            rows = pl.ds(pl.multiple_of(i * F, 128), F)
            pltpu.make_async_copy(s_down.at[rows, cols], ring_d.at[slot], sem_d.at[slot]).start()

    def wait_dn(slot):
        pltpu.make_async_copy(w_down.at[0, :, pl.ds(0, CHUNK)], ring_d.at[slot], sem_d.at[slot]).wait()

    def x_load(k):
        return pltpu.make_async_copy(tok.at[:, pl.ds(k * CHUNK, CHUNK)], xall.at[k, me], sem_x.at[k])

    for k in range(KC):
        x_load(k).start()
    for g in range(RING1 - 1):
        issue_gu(jnp.int32(g), n_gu)

    barrier = pltpu.get_barrier_semaphore()
    for dev in (pp, qq, rr):
        pl.semaphore_signal(barrier, inc=1, device_id={"ep": dev}, device_id_type=MESH)

    ids = ids_ref[...]
    gat = gat_ref[...]
    row = lax.broadcasted_iota(jnp.int32, (GROUP * 16, T), 0)
    low = jnp.bitwise_and(row, 15)
    ident = jnp.where(low < L, jnp.right_shift(row, 4) * L + low, -2)
    chosen = jnp.zeros((GROUP * 16, T), F32)
    gates = jnp.zeros((GROUP * 16, T), F32)
    for j in range(4):
        hit = ids[j:j + 1, :] == ident
        chosen = jnp.where(hit, 1.0, chosen)
        gates = jnp.where(hit, gat[j:j + 1, :], gates)
    before = (lax.broadcasted_iota(jnp.int32, (T, T), 0) < lax.broadcasted_iota(jnp.int32, (T, T), 1))
    place = dot(chosen.astype(BF16), jnp.where(before, 1.0, 0.0).astype(BF16))
    place = jnp.where(chosen > 0.5, place, -1.0)
    for d in range(GROUP):
        meta_loc[d, 0:16, :] = place[d * 16:(d + 1) * 16, :]
        meta_loc[d, 16:32, :] = gates[d * 16:(d + 1) * 16, :]

    pl.semaphore_wait(barrier, 3)

    def x_to_q(k, src):
        return remote(xall.at[k, src], xall.at[k, src], xq_s.at[k], xq_r.at[k], qq)

    def x_to_p(k, src):
        return remote(xall.at[k, src], xall.at[k, src], xp_s.at[k], xp_r.at[k], pp)

    def x_fwd(k, src):
        return remote(xall.at[k, src], xall.at[k, src], xf_s.at[k], xf_r.at[k], pp)

    def meta_to(which, dev, src):
        return remote(meta_loc.at[dev], meta_all.at[src], meta_s.at[which], meta_r.at[which], dev)

    for k in range(KC):
        x_load(k).wait()
        x_to_q(k, me).start()
        x_to_p(k, me).start()
    peers = (pp, qq, rr)
    for which, dev in enumerate(peers):
        meta_to(which, dev, me).start()
    meta_all[me] = meta_loc[me]
    ybuf[...] = jnp.zeros(ybuf.shape, F32)

    def silu_mul(g, u):
        return ((g * jax.nn.sigmoid(g)) * u).astype(BF16)

    def gu_step(slot, lhs, acc_ref, row0, rows, k):
        for start, width in pieces(F):
            old_g = acc_ref[pl.ds(row0, rows), pl.ds(start, width)]
            acc_ref[pl.ds(row0, rows), pl.ds(start, width)] = jnp.where(k > 0, old_g, 0.0) + dot(
                lhs, ring_g[slot, :, pl.ds(start, width)])
            old_u = acc_ref[pl.ds(row0, rows), pl.ds(F + start, width)]
            acc_ref[pl.ds(row0, rows), pl.ds(F + start, width)] = jnp.where(k > 0, old_u, 0.0) + dot(
                lhs, ring_u[slot, :, pl.ds(start, width)])

    def shared_gu(idx, g):
        slot = lax.rem(g, RING1)
        i, k = idx // KC, lax.rem(idx, KC)
        wait_gu(slot)
        gu_step(slot, xall[k, me], sacc, 0, T, k)

        @pl.when(k == KC - 1)
        def _():
            for start, width in pieces(F):
                shid[i, :, pl.ds(start, width)] = silu_mul(sacc[:, pl.ds(start, width)], sacc[:, pl.ds(F + start, width)])

    def cover_body(g, carry):
        issue_gu(g + RING1 - 1, n_cover + n_routed)
        shared_gu(g, g)
        return carry

    lax.fori_loop(0, n_cover, cover_body, 0)

    for which, dev in enumerate(peers):
        meta_to(which, dev, dev).wait_recv()

    slot_row = lax.broadcasted_iota(jnp.int32, (SLOTS, T), 0).astype(F32)

    def tables(s, carry):
        for grp in range(NGRP):
            blocks = []
            for j in range(EGROUP):
                e = grp * EGROUP + j
                hit = meta_all[s, e:e + 1, :] == slot_row
                blocks.append(jnp.where(hit, 1.0, 0.0))
                ybuf[0, e * SLOTS:(e + 1) * SLOTS, 0:T] = jnp.where(hit, meta_all[s, 16 + e:17 + e, :], 0.0)
            blocks.append(jnp.zeros((8, T), F32))
            pmat[s, grp] = jnp.concatenate(blocks, axis=0).astype(BF16)
        for start in range(0, 640, 128):
            g = ybuf[0, start:start + 128, 0:T].T
            hi = g.astype(BF16)
            rest = g - hi.astype(F32)
            mid = rest.astype(BF16)
            gmat[0, s, :, start:start + 128] = hi
            gmat[1, s, :, start:start + 128] = mid
            gmat[2, s, :, start:start + 128] = (rest - mid.astype(F32)).astype(BF16)
        return carry

    lax.fori_loop(0, GROUP, tables, 0)

    def routed_body(gk, carry):
        grp, k = gk // KC, lax.rem(gk, KC)

        @pl.when(grp == 0)
        def _():
            x_to_q(k, qq).wait_recv()
            x_fwd(k, qq).start()
            x_to_p(k, pp).wait_recv()
            x_fwd(k, rr).wait_recv()

        @pl.when(gk == NGRP * KC - 1)
        def _():
            for t in range(RING2 - 1):
                issue_dn(jnp.int32(t), n_down)

        for s in range(GROUP):
            lhs = pmat[s, grp]
            for start, width in pieces(CHUNK):
                rows = dot(lhs, xall[k, s, :, pl.ds(start, width)])
                for j in range(EGROUP):
                    xdf[j * ROWS + s * SLOTS:j * ROWS + (s + 1) * SLOTS, pl.ds(start, width)] = rows[j * SLOTS:(j + 1) * SLOTS, :]
        xd[...] = xdf[...].astype(BF16)

        def expert(j, c):
            g = n_cover + gk * EGROUP + j
            issue_gu(g + RING1 - 1, n_cover + n_routed)
            slot = lax.rem(g, RING1)
            wait_gu(slot)
            row0 = pl.multiple_of(j * ROWS, ROWS)
            gu_step(slot, xd[pl.ds(row0, ROWS), :], acc, row0, ROWS, k)

            @pl.when(k == KC - 1)
            def _():
                for start, width in pieces(F):
                    hid[grp * EGROUP + j, :, pl.ds(start, width)] = silu_mul(
                        acc[pl.ds(row0, ROWS), pl.ds(start, width)], acc[pl.ds(row0, ROWS), pl.ds(F + start, width)])
            return c

        lax.fori_loop(0, EGROUP, expert, 0)
        return carry

    lax.fori_loop(0, NGRP * KC, routed_body, 0)
    ybuf[...] = jnp.zeros(ybuf.shape, F32)

    def cf(n):
        return remote(acc.at[pl.ds(0, T), pl.ds(pl.multiple_of(n * CHUNK, CHUNK), CHUNK)], recv_f.at[n], cf_s.at[n], cf_r.at[n], pp)

    def cp(n):
        return remote(acc.at[pl.ds(T, T), pl.ds(pl.multiple_of(n * CHUNK, CHUNK), CHUNK)], recv_p.at[n], cp_s.at[n], cp_r.at[n], pp)

    def cq(n):
        return remote(recv_f.at[n], recv_q.at[n], cq_s.at[n], cq_r.at[n], qq)

    def partial(s, start, width):
        y = ybuf[s, :, pl.ds(start, width)].astype(BF16)
        return dot(gmat[0, s], y) + dot(gmat[1, s], y) + dot(gmat[2, s], y)

    def down_body(n, carry):
        def expert(e, c):
            t = n * L + e
            issue_dn(t + RING2 - 1, n_down)
            slot = lax.rem(t, RING2)
            wait_dn(slot)
            h = hid[e]
            for start, width in pieces(CHUNK):
                y = dot(h, ring_d[slot, :, pl.ds(start, width)]).astype(BF16).astype(F32)
                for s in range(GROUP):
                    ybuf[s, pl.ds(pl.multiple_of(e * SLOTS, 8), SLOTS), pl.ds(start, width)] = y[s * SLOTS:(s + 1) * SLOTS, :]
            return c

        lax.fori_loop(0, L, expert, 0)

        @pl.when(n == KC - 1)
        def _():
            for g in range(RING1 - 1):
                issue_gu(jnp.int32(n_cover + n_routed + g), n_gu)

        col = pl.multiple_of(n * CHUNK, CHUNK)
        for start, width in pieces(CHUNK):
            acc[pl.ds(0, T), pl.ds(col + start, width)] = partial(rr, start, width)
        cf(n).start()
        for start, width in pieces(CHUNK):
            acc[pl.ds(T, T), pl.ds(col + start, width)] = partial(pp, start, width)
        cp(n).start()
        for start, width in pieces(CHUNK):
            acc[pl.ds(2 * T, T), pl.ds(col + start, width)] = partial(me, start, width)
        cf(n).wait_recv()
        for start, width in pieces(CHUNK):
            recv_f[n, :, pl.ds(start, width)] = recv_f[n, :, pl.ds(start, width)] + partial(qq, start, width)
        cq(n).start()
        return carry

    lax.fori_loop(0, KC, down_body, 0)

    for t in range(RING2 - 1):
        issue_dn(jnp.int32(n_down + t), n_dn)

    def rest_body(idx, carry):
        g = n_routed + idx
        issue_gu(g + RING1 - 1, n_gu)
        shared_gu(idx, g)
        return carry

    lax.fori_loop(n_cover, NS * KC, rest_body, 0)

    def shared_down(n, carry):
        col = pl.multiple_of(n * CHUNK, CHUNK)

        def block(i, c):
            t = n_down + n * NS + i
            issue_dn(t + RING2 - 1, n_dn)
            slot = lax.rem(t, RING2)
            wait_dn(slot)
            h = shid[i]
            for start, width in pieces(CHUNK):
                old = sacc[:, pl.ds(start, width)]
                sacc[:, pl.ds(start, width)] = jnp.where(i > 0, old, 0.0) + dot(h, ring_d[slot, :, pl.ds(start, width)])
            return c

        lax.fori_loop(0, NS, block, 0)
        acc[pl.ds(2 * T, T), pl.ds(col, CHUNK)] = acc[pl.ds(2 * T, T), pl.ds(col, CHUNK)] + (
            sacc[:, 0:CHUNK].astype(BF16).astype(F32) + xall[n, me].astype(F32))
        return carry

    lax.fori_loop(0, KC, shared_down, 0)

    def store(n):
        return pltpu.make_async_copy(out_v.at[n], out.at[:, pl.ds(pl.multiple_of(n * CHUNK, CHUNK), CHUNK)], sem_o.at[n])

    def finish(n, carry):
        col = pl.multiple_of(n * CHUNK, CHUNK)
        cp(n).wait_recv()
        cq(n).wait_recv()
        out_v[n] = (acc[pl.ds(2 * T, T), pl.ds(col, CHUNK)] + recv_p[n] + recv_q[n]).astype(BF16)
        store(n).start()
        return carry

    lax.fori_loop(0, KC, finish, 0)

    for k in range(KC):
        x_to_q(k, me).wait_send()
        x_to_p(k, me).wait_send()
        x_fwd(k, qq).wait_send()
        cf(k).wait_send()
        cp(k).wait_send()
        cq(k).wait_send()
        store(k).wait()
    for which, dev in enumerate(peers):
        meta_to(which, dev, me).wait_send()


def solution(mesh):
    assert mesh.shape["ep"] == GROUP

    def moe_step(tokens, expert_ids, gate_vals, w_gate, w_up, w_down, shared_gate, shared_up, shared_down):
        T, D = tokens.shape
        L, _, F = w_gate.shape
        NS = shared_gate.shape[1] // F
        KC = D // CHUNK
        ROWS = GROUP * SLOTS
        top = expert_ids.shape[1]
        ids_t = jnp.pad(expert_ids.T, ((0, 8 - top), (0, 0)), constant_values=-1)
        gat_t = jnp.pad(gate_vals.T, ((0, 8 - top), (0, 0)))
        vmem = pl.BlockSpec(memory_space=pltpu.VMEM)
        hbm = pl.BlockSpec(memory_space=pl.ANY)
        dma = pltpu.SemaphoreType.DMA
        return pl.pallas_call(
            functools.partial(moe_kernel, (T, D, F, L, NS)),
            out_shape=jax.ShapeDtypeStruct((T, D), BF16),
            in_specs=[vmem, vmem] + [hbm] * 7,
            out_specs=hbm,
            scratch_shapes=[
                pltpu.VMEM((RING1, CHUNK, F), BF16),
                pltpu.VMEM((RING1, CHUNK, F), BF16),
                pltpu.VMEM((RING2, F, CHUNK), BF16),
                pltpu.VMEM((EGROUP * ROWS, 2 * F), F32),
                pltpu.VMEM((T, 2 * F), F32),
                pltpu.VMEM((KC, GROUP, T, CHUNK), BF16),
                pltpu.VMEM((EGROUP * ROWS, CHUNK), F32),
                pltpu.VMEM((EGROUP * ROWS, CHUNK), BF16),
                pltpu.VMEM((GROUP, 640, CHUNK), F32),
                pltpu.VMEM((L, ROWS, F), BF16),
                pltpu.VMEM((NS, T, F), BF16),
                pltpu.VMEM((3, GROUP, T, 640), BF16),
                pltpu.VMEM((GROUP, L // EGROUP, EGROUP * SLOTS + 8, T), BF16),
                pltpu.VMEM((KC, T, CHUNK), F32),
                pltpu.VMEM((KC, T, CHUNK), F32),
                pltpu.VMEM((KC, T, CHUNK), F32),
                pltpu.VMEM((KC, T, CHUNK), BF16),
                pltpu.VMEM((GROUP, 32, T), F32),
                pltpu.VMEM((GROUP, 32, T), F32),
                dma((RING1,)), dma((RING1,)), dma((RING2,)), dma((KC,)), dma((KC,)), dma((3,)), dma((3,)),
                dma((KC,)), dma((KC,)), dma((KC,)), dma((KC,)), dma((KC,)), dma((KC,)),
                dma((KC,)), dma((KC,)), dma((KC,)), dma((KC,)), dma((KC,)), dma((KC,)),
            ],
            compiler_params=pltpu.CompilerParams(
                collective_id=0, has_side_effects=True, vmem_limit_bytes=67043328),
        )(ids_t, gat_t, tokens, w_gate, w_up, w_down, shared_gate, shared_up, shared_down)

    row_spec = P(("dp", "ep"), None)
    expert_spec = P("ep", None, None)
    whole_spec = P(None, None)
    return jax.shard_map(moe_step, mesh=mesh, in_specs=(row_spec, row_spec, row_spec, expert_spec, expert_spec, expert_spec, whole_spec, whole_spec, whole_spec), out_specs=row_spec, check_vma=False)
```
